512 devices in a mesh: groups: 2 (over y), seq: 32 (over z), sample: 4 (over x), vocab: 2 (over core).
Axes of the slice: x: 4, y: 2, z: 32, core: 2. Of those that a mesh axis runs over, the one named last changes fastest.
The devices are a block of a 4x8x32 slice.
Arguments:
- queries: bfloat16 [16, 2048, 1792], P(('groups', 'sample'), 'seq', 'vocab'), parts along dimension 0, may hold values from -130 to 130
- key_states: bfloat16 [16, 2048, 256], P(('groups', 'sample'), 'seq', 'vocab'), parts along dimension 0, may hold values from -8 to 8
- value_states: bfloat16 [16, 2048, 256], P(('groups', 'sample'), 'seq', 'vocab'), parts along dimension 0, may hold values from -6 to 6
- residual: bfloat16 [16, 2048, 1792], P(('groups', 'sample'), 'seq'), parts along dimension 0, may hold values from -3 to 3
- out_weight: bfloat16 [1792, 1792], P('vocab'), may hold values from -0.5 to 0.5
- norm_gain: float32 [1792], replicated, may hold values from 0.5 to 1.5
- vocab_head: bfloat16 [81920, 1792], P(('seq', 'sample', 'vocab')), may hold values from -21 to 21
- targets: int32 [16, 2048], P(('groups', 'sample')), parts along dimension 0, may hold values from 0 to 81919
- scored_slots: int32 [16, 512], P(('groups', 'sample')), parts along dimension 0, may hold values from -1 to 2047, as said below
- lengths: int32 [16], P(('groups', 'sample')), parts along dimension 0, may hold values from 512 to 2048
- rewards: int32 [16], P(('groups', 'sample')), parts along dimension 0, may hold values from 0 to 4
Outputs:
- token_logprobs: float32 [16, 512], P(('groups', 'sample'), 'seq'), parts along dimension 0
- seq_scores: float32 [16], P(('groups', 'sample')), parts along dimension 0
- advantages: float32 [16], P(('groups', 'sample')), parts along dimension 0
- objective: float32 [2], P('groups'), parts along dimension 0
The draws below stay inside these ranges and needn't reach their ends.
There are 2 independent parts, one for each index of `groups`. The reference program is written for one: setup_inputs(seed, part) draws one part's arguments, and reference() takes and returns one part's arrays. A program takes and returns all parts, laid end to end along the dimension named above; an argument that names none is the same for every part. Nothing has to cross between parts.
Inputs may be any that keep to these rules, and one draw needn't show every extreme that they name: `scored_slots`: slots b * 16 to (b + 1) * 16 - 1 of a completion hold distinct positions of b * 64 to (b + 1) * 64 - 1 in rising order, followed by -1 in unused slots; every completion fills all 16 slots of some block; positions not listed are not scored. Positions from lengths[i] on are padding.
All inputs are finite; a program needn't handle non-finite values.
Results may differ from the reference program's by a relative error of at most 0.0085.
Values may be sent and summed in bfloat16 or wider, within the bound.
A program may use at most 64 MiB of HBM per device.

```python
import math
import jax
import jax.numpy as jnp
import numpy as np
from jax import lax

D = 1792
HQ = 14
HK = 2
HD = 128
V = 81920
K = 8
CH = 64
L = 2048
CAP = 16


def attention_inputs(key):
    query_draw = jnp.clip(jax.random.normal(jax.random.fold_in(key, 11), (K, L, HQ * HD), jnp.float32), -6.0, 6.0)
    key_draw = jnp.clip(jax.random.normal(jax.random.fold_in(key, 12), (K, L, HK * HD), jnp.float32), -6.0, 6.0)
    return (query_draw, key_draw)


def draw_queries(key, part):
    return attention_inputs(key)[0].astype(jnp.bfloat16)


def draw_key_states(key, part):
    return attention_inputs(key)[1].astype(jnp.bfloat16)


def draw_vocab_head(key, part):
    base = jnp.clip(jax.random.normal(jax.random.fold_in(key, 21), (V, D), jnp.float32), -6.0, 6.0) * (3.0 / math.sqrt(D))
    return base.astype(jnp.bfloat16)


def draw_scored_slots(key, part):
    blocks = L // CH
    full_block = jax.random.randint(jax.random.fold_in(key, 31), (K,), 0, blocks)
    counts = jax.random.randint(jax.random.fold_in(key, 32), (K, blocks), CAP // 3, CAP + 1)
    counts = jnp.where(jnp.arange(blocks)[None, :] == full_block[:, None], CAP, counts)
    block_keys = jax.random.split(jax.random.fold_in(key, 33), K * blocks)
    picks = jax.vmap(lambda one_key: jnp.sort(jax.random.permutation(one_key, CH)[:CAP]))(block_keys)
    positions = picks.reshape(K, blocks, CAP) + (jnp.arange(blocks) * CH)[None, :, None]
    used = jnp.arange(CAP)[None, None, :] < counts[:, :, None]
    return jnp.where(used, positions, -1).reshape(K, blocks * CAP).astype(jnp.int32)


def with_ends(values, rng, least, largest):
    dims = values.shape
    spot = [jax.random.randint(jax.random.fold_in(rng, axis), (), 0, dims[axis]) for axis in range(len(dims))]
    values = values.at[tuple(spot)].set(least)
    longest = dims.index(max(dims))
    spot[longest] = (spot[longest] + 1) % dims[longest]
    return values.at[tuple(spot)].set(largest)


def shard_levels(own_key, extent, cuts, smallest, high):
    def one(axis_at, blocks):
        steps = jax.random.uniform(jax.random.fold_in(jax.random.fold_in(own_key, 6), axis_at), (blocks,), jnp.float32, smallest / len(cuts), high / len(cuts))
        return jnp.repeat(jnp.exp(steps), extent[axis_at] // blocks).reshape((-1,) + (1,) * (len(extent) - axis_at - 1))

    level = one(*cuts[0])
    for cut in cuts[1:]:
        level = level * one(*cut)
    return level


def skewed_wide(rng, extent, amount, slope):
    weights = [min(1 << octave, amount + 1 - (1 << octave)) * (1 << 20) // math.isqrt((1 << octave) ** slope) + 1 for octave in range((amount + 1).bit_length()) if 1 << octave <= amount]
    scale = 1 + sum(weights) // (1 << 30)
    table = np.cumsum(np.array([max(1, weight // scale) for weight in weights]))
    pick = jax.random.randint(jax.random.fold_in(rng, 1), extent, 0, int(table[len(weights) - 1]))
    start = jnp.left_shift(1, jnp.searchsorted(jnp.asarray(table, jnp.int32), pick, side="right").astype(jnp.int32))
    standing = start - 1 + jax.random.randint(jax.random.fold_in(rng, 4), extent, 0, 1 << 30) % jnp.minimum(start, amount + 1 - start)
    return jax.random.permutation(jax.random.fold_in(rng, 2), amount)[standing].astype(jnp.int32)


def scatter_about(own_key, shape, scale, reach, cuts=(), kind=jnp.bfloat16):
    gain = shard_levels(own_key, shape, cuts, -0.22, 0.18) if cuts else 1.0
    entries = jax.random.normal(own_key, shape, jnp.float32) * scale * gain
    return jnp.minimum(jnp.maximum(entries, -reach), reach).astype(kind)


def setup_inputs(seed: int = 0, part: int = 0) -> dict:
    key_list = jax.random.split(jax.random.key(seed), 12)
    own_keys = jax.random.split(jax.random.fold_in(key_list[11], part), 12)
    return {
        "queries": draw_queries(jax.random.fold_in(jax.random.fold_in(key_list[11], part), 71), part),
        "key_states": draw_key_states(jax.random.fold_in(jax.random.fold_in(key_list[11], part), 71), part),
        "value_states": scatter_about(own_keys[2], (K, L, HK * HD), 1.0, 6.0, ((0, 4), (1, 32), (2, 2))),
        "residual": scatter_about(own_keys[3], (K, L, D), 0.5, 3.0, ((0, 4), (1, 32))),
        "out_weight": scatter_about(key_list[4], (HQ * HD, D), (HQ * HD // 16) ** -0.5, 0.5, ((0, 2),)),
        "norm_gain": jnp.clip(1.0 + 0.1 * jax.random.normal(key_list[5], (D,), jnp.float32), 0.5, 1.5),
        "vocab_head": draw_vocab_head(jax.random.fold_in(key_list[11], 71), part),
        "targets": with_ends(skewed_wide(own_keys[7], (K, L), V, 2), jax.random.fold_in(own_keys[7], 3), 0, V - 1).astype(jnp.int32),
        "scored_slots": draw_scored_slots(jax.random.fold_in(jax.random.fold_in(key_list[11], part), 71), part),
        "lengths": with_ends(jax.random.randint(own_keys[9], (K,), L // 4, L + 1), jax.random.fold_in(own_keys[9], 1), L // 4, L).astype(jnp.int32),
        "rewards": with_ends(jax.random.randint(own_keys[10], (K,), 0, 5), jax.random.fold_in(own_keys[10], 1), 0, 4).astype(jnp.int32),
    }


def attend_sample(inputs):
    query_rows, key_rows, value_rows = inputs
    seq_len = query_rows.shape[0]
    group_size = HQ // HK
    query_view = query_rows.reshape(seq_len, HK, group_size, HD).astype(jnp.float32)
    key_view = key_rows.reshape(seq_len, HK, HD).astype(jnp.float32)
    value_view = value_rows.reshape(seq_len, HK, HD).astype(jnp.float32)
    scores = jnp.einsum('tkgd,skd->tkgs', query_view, key_view) * HD ** (-0.5)
    positions = jnp.arange(seq_len, dtype=jnp.int32)
    allowed = (positions[None, :] <= positions[:, None])[:, None, None, :]
    masked = jnp.where(allowed, scores, -1e+30)
    top_score = lax.optimization_barrier(jnp.max(masked, axis=-1, keepdims=True))
    exponent = jnp.where(allowed, jnp.exp(masked - top_score), 0.0)
    weight_sum = lax.optimization_barrier(jnp.sum(exponent, axis=-1))
    rounded = lax.optimization_barrier(exponent.astype(jnp.bfloat16))
    mixed = jnp.einsum('tkgs,skd->tkgd', rounded.astype(jnp.float32), value_view)
    return (mixed / weight_sum[..., None]).reshape(seq_len, HQ * HD).astype(jnp.bfloat16)

def score_rows(normed_rows, wanted, vocab_head):
    logits = jnp.dot(normed_rows, vocab_head.T, preferred_element_type=jnp.float32)
    top_score = lax.optimization_barrier(jnp.max(logits, axis=-1))
    weight_sum = lax.optimization_barrier(jnp.sum(jnp.exp(logits - top_score[:, None]), axis=-1))
    picked = jnp.take_along_axis(logits, wanted[:, None].astype(jnp.int32), axis=1)[:, 0]
    return picked - (top_score + jnp.log(weight_sum))

def reference(queries, key_states, value_states, residual, out_weight, norm_gain, vocab_head, targets, scored_slots, lengths, rewards):
    attended = lax.map(attend_sample, (queries, key_states, value_states))
    sample_count, seq_len, model_width = residual.shape
    partial_value = jnp.dot(attended.reshape(sample_count * seq_len, HQ * HD), out_weight, preferred_element_type=jnp.float32)
    hidden = residual.reshape(sample_count * seq_len, model_width).astype(jnp.float32) + partial_value
    power = lax.optimization_barrier(jnp.mean(hidden * hidden, axis=-1, keepdims=True))
    normed = (hidden * lax.rsqrt(power + 1e-06) * norm_gain).astype(jnp.bfloat16)
    normed = normed.reshape(sample_count, seq_len, model_width)
    slot_pos = jnp.maximum(scored_slots, 0).astype(jnp.int32)
    chosen = jnp.take_along_axis(normed, slot_pos[:, :, None], axis=1)
    wanted = jnp.take_along_axis(targets, slot_pos, axis=1)
    logprob = lax.map(lambda pair: score_rows(pair[0], pair[1], vocab_head), (chosen, wanted))
    scored = (scored_slots >= 0) & (scored_slots < lengths[:, None])
    token_logprobs = jnp.where(scored, logprob, 0.0)
    seq_scores = lax.optimization_barrier(jnp.sum(token_logprobs, axis=-1)) / seq_len
    reward_vals = rewards.astype(jnp.float32)
    reward_sum = jnp.sum(reward_vals)
    advantages = reward_vals - (reward_sum - reward_vals) / (K - 1)
    objective = -(jnp.sum(advantages * seq_scores) / K).reshape(1)
    return (token_logprobs, seq_scores, advantages, objective)
```

```python
import functools

import jax
import jax.numpy as jnp
from jax import lax
from jax.experimental import pallas as pl
from jax.experimental.pallas import tpu as pltpu
from jax.sharding import PartitionSpec as P

HD = 128
LANES = 128
STEP = 4
FLOOR = -1e30
NT = (((1,), (1,)), ((), ()))
MESH = pl.DeviceIdType.MESH
F32 = jnp.float32
BF16 = jnp.bfloat16


def kernel(
    nz,
    nx,
    full_len,
    info_ref,
    len_ref,
    rew_ref,
    gain_ref,
    q_hbm,
    k_hbm,
    v_hbm,
    res_hbm,
    w_hbm,
    head_hbm,
    tok_ref,
    seq_ref,
    adv_ref,
    obj_ref,
    q_buf,
    res_buf,
    w_buf,
    head,
    kv,
    nrm,
    q_rows,
    res_rows,
    top_buf,
    sum_buf,
    acc_buf,
    part,
    part_in,
    stat,
    stat_out,
    stat_in,
    line,
    x_in,
    z_out,
    z_in,
    load_sem,
    head_send,
    head_recv,
    kv_send,
    kv_recv,
    nrm_send,
    nrm_recv,
    mate_send,
    mate_recv,
    part_send,
    part_recv,
    stat_send,
    stat_recv,
    x_send,
    x_recv,
    z_send,
    z_recv,
):
    z = lax.axis_index("seq")
    x = lax.axis_index("sample")
    c = lax.axis_index("vocab")
    half = nz // 2
    own = nz - 1
    block_len = q_buf.shape[1]
    slots = nrm.shape[2]
    group = q_buf.shape[2] // HD
    width = nrm.shape[3]
    rows = head.shape[1]
    cut = width // 2
    z_up, z_down = lax.rem(z + 1, nz), lax.rem(z + nz - 1, nz)
    mate = {"vocab": 1 - c}

    def up(s):
        return (s - 1) // STEP * (2 * STEP) + (s - 1) % STEP

    def down(s):
        return up(s) + STEP

    def send(src, dst, send_sem, recv_sem, where):
        return pltpu.make_async_remote_copy(
            src_ref=src,
            dst_ref=dst,
            send_sem=send_sem,
            recv_sem=recv_sem,
            device_id=where,
            device_id_type=MESH,
        )

    loads = [
        pltpu.make_async_copy(k_hbm, kv.at[own, 0], load_sem.at[0]),
        pltpu.make_async_copy(v_hbm, kv.at[own, 1], load_sem.at[1]),
        pltpu.make_async_copy(head_hbm, head.at[0], load_sem.at[2]),
        pltpu.make_async_copy(q_hbm, q_buf, load_sem.at[3]),
        pltpu.make_async_copy(res_hbm.at[c], res_buf, load_sem.at[4]),
        pltpu.make_async_copy(w_hbm, w_buf, load_sem.at[5]),
    ]
    for load in loads:
        load.start()
    barrier = pltpu.get_barrier_semaphore()
    peers = [{"seq": z_up}, {"seq": z_down}, mate]
    peers += [{"sample": lax.rem(x + d, nx)} for d in range(1, nx)]
    for peer in peers:
        pl.semaphore_signal(barrier, inc=1, device_id=peer, device_id_type=MESH)
    pl.semaphore_wait(barrier, len(peers))

    def kv_copy(src, dst, part_no, where):
        return send(
            kv.at[src, part_no],
            kv.at[dst, part_no],
            kv_send.at[dst, part_no],
            kv_recv.at[dst, part_no],
            {"seq": where},
        )

    for i in range(2):
        loads[i].wait()
        kv_copy(own, up(1), i, z_up).start()
        kv_copy(own, down(1), i, z_down).start()

    hx = rows // 2
    right, left = {"sample": lax.rem(x + 1, nx)}, {"sample": lax.rem(x + nx - 1, nx)}

    def head_copy(src, dst, lo, n, where):
        return send(
            head.at[src, pl.ds(lo, hx)],
            head.at[dst, pl.ds(lo, hx)],
            head_send.at[n],
            head_recv.at[n],
            where,
        )

    loads[2].wait()
    to_right = [head_copy(0, 3, 0, 0, right), head_copy(0, 3, hx, 1, right)]
    to_left = [head_copy(0, 1, hx, 2, left), head_copy(0, 1, 0, 3, left)]
    pass_right = head_copy(3, 2, 0, 4, right)
    pass_left = head_copy(1, 2, hx, 5, left)
    for a, b in zip(to_right, to_left):
        a.start()
        b.start()

    lane = lax.broadcasted_iota(jnp.int32, (1, LANES), 1)
    own_info = info_ref[z]

    def picker(e):
        wide = jnp.broadcast_to(own_info, (slots, LANES))
        at = lax.broadcasted_iota(jnp.int32, (slots, LANES), 0) + (2 * slots + e * slots)
        spot = jnp.sum(
            jnp.where(lax.broadcasted_iota(jnp.int32, (slots, LANES), 1) == at, wide, 0),
            axis=1,
            keepdims=True,
        )
        local = jnp.clip(spot - z * block_len, 0, block_len - 1)
        hot = lax.broadcasted_iota(jnp.int32, (slots, block_len), 1) == local
        return hot.astype(F32).astype(BF16), local

    picks = [picker(e) for e in range(2)]
    loads[3].wait()
    for e in range(2):
        rows_e = jnp.dot(picks[e][0], q_buf[e], preferred_element_type=F32).astype(BF16)
        for h in range(group):
            q_rows[e, pl.ds(h * slots, slots), :] = rows_e[:, h * HD : (h + 1) * HD]
    loads[4].wait()
    own_pick = jnp.where(c == 0, picks[0][0].astype(F32), picks[1][0].astype(F32)).astype(BF16)
    res_rows[...] = jnp.dot(own_pick, res_buf[...], preferred_element_type=F32)

    scale = HD ** (-0.5)
    for e in range(2):
        s0 = lax.dot_general(q_rows[e], kv[own, 0, e], NT, preferred_element_type=F32) * scale
        spot = jnp.concatenate([picks[e][1]] * group, axis=0)
        ok = lax.broadcasted_iota(jnp.int32, s0.shape, 1) <= spot
        s0 = jnp.where(ok, s0, FLOOR)
        top = jnp.max(s0, axis=1, keepdims=True)
        w0 = jnp.where(ok, jnp.exp(s0 - top), 0.0)
        top_buf[e] = jnp.broadcast_to(top, top_buf.shape[1:])
        sum_buf[e] = jnp.broadcast_to(jnp.sum(w0, axis=1, keepdims=True), sum_buf.shape[1:])
        acc_buf[e] = jnp.dot(w0.astype(BF16), kv[own, 1, e], preferred_element_type=F32)

    def attend(first):
        span = 2 * STEP * block_len
        piece = lax.broadcasted_iota(jnp.int32, (1, span), 1) // block_len
        off = first // 2 + 1 + piece % STEP
        is_up = piece < STEP
        ok = jnp.where(is_up, off - z, 1 - jnp.where(off < half, z + off - nz + 1, 0)) <= 0
        for e in range(2):
            keys = kv[pl.ds(first, 2 * STEP), 0, e].reshape(span, HD)
            vals = kv[pl.ds(first, 2 * STEP), 1, e].reshape(span, HD)
            sc = lax.dot_general(q_rows[e], keys, NT, preferred_element_type=F32) * scale
            sc = jnp.where(ok, sc, FLOOR)
            old = top_buf[e][:, :1]
            top = jnp.maximum(old, jnp.max(sc, axis=1, keepdims=True))
            wt = jnp.exp(sc - top)
            fade = jnp.exp(old - top)
            total = sum_buf[e][:, :1] * fade + jnp.sum(wt, axis=1, keepdims=True)
            acc_buf[e] = acc_buf[e] * fade + jnp.dot(
                wt.astype(BF16), vals, preferred_element_type=F32
            )
            top_buf[e] = jnp.broadcast_to(top, top_buf.shape[1:])
            sum_buf[e] = jnp.broadcast_to(total, sum_buf.shape[1:])

    def kv_step(i, carry):
        s = i + 1
        for n in range(2):
            kv_copy(own, up(s), n, z_up).wait_recv()

            @pl.when(s < half)
            def _():
                kv_copy(up(s), up(s + 1), n, z_up).start()
                kv_copy(own, down(s), n, z_down).wait_recv()

            @pl.when(s < half - 1)
            def _():
                kv_copy(down(s), down(s + 1), n, z_down).start()

        @pl.when(s == half // 2)
        def _():
            to_right[0].wait_recv()
            pass_right.start()
            to_left[0].wait_recv()
            pass_left.start()

        @pl.when(s % STEP == 0)
        def _():
            attend((s - 1) // STEP * (2 * STEP))

        return carry

    lax.fori_loop(0, half, kv_step, 0)

    sides = []
    for e in range(2):
        att = (acc_buf[e] / sum_buf[e]).astype(BF16)
        sides.append(
            jnp.concatenate([att[h * slots : (h + 1) * slots] for h in range(group)], axis=1)
        )
    loads[5].wait()
    both = jnp.dot(jnp.concatenate(sides, axis=0), w_buf[...], preferred_element_type=F32)
    for e in range(2):
        part[e] = both[e * slots : (e + 1) * slots]
    swap = send(part.at[1 - c], part_in, part_send, part_recv, mate)
    swap.start()
    hidden = res_rows[...] + part[c]
    swap.wait_recv()
    hidden = hidden + part_in[...]
    power = jnp.mean(hidden * hidden, axis=1, keepdims=True)
    nrm[own, c] = (hidden * lax.rsqrt(power + 1e-06) * gain_ref[...]).astype(BF16)

    def nrm_copy(src, dst, n, where):
        at = pl.ds(n * cut, cut)
        return send(
            nrm.at[src, c, :, at],
            nrm.at[dst, c, :, at],
            nrm_send.at[dst, n],
            nrm_recv.at[dst, n],
            {"seq": where},
        )

    def mate_copy(slot, e):
        return send(nrm.at[slot, e], nrm.at[slot, e], mate_send.at[slot], mate_recv.at[slot], mate)

    for n in range(2):
        nrm_copy(own, up(1), n, z_up).start()
        nrm_copy(own, down(1), n, z_down).start()
    mate_copy(own, c).start()
    to_right[1].wait_recv()
    to_left[1].wait_recv()
    pass_right.wait_recv()
    pass_left.wait_recv()

    def origin(slot):
        s = slot // (2 * STEP) * STEP + slot % STEP + 1
        move = jnp.where(slot % (2 * STEP) < STEP, nz - s, jnp.where(slot == own, 0, s))
        return lax.rem(z + move, nz)

    def scored(first, j):
        batch = nrm[pl.ds(first, 2 * STEP)].reshape(2 * STEP * 2 * slots, width)
        logits = lax.dot_general(head[j], batch, NT, preferred_element_type=F32)
        base = ((z * nx + lax.rem(x + j, nx)) * 2 + c) * rows
        ids = lax.broadcasted_iota(jnp.int32, logits.shape, 0) + base
        want = []
        per = LANES // (2 * slots)
        for t in range(2 * STEP // per):
            lines = info_ref[origin(first + t * per)]
            for i in range(1, per):
                moved = pltpu.roll(info_ref[origin(first + t * per + i)], i * 2 * slots, 1)
                lines = jnp.where(lane < i * 2 * slots, lines, moved)
            want.append(lines)
        want = jnp.concatenate(want, axis=1)
        hit = jnp.sum(jnp.where(ids == want, logits, 0.0), axis=0, keepdims=True)
        fresh = jnp.where(j == 0, 0.0, 1.0)
        old = jnp.where(j == 0, FLOOR, stat[0])
        top = jnp.maximum(old, jnp.max(logits, axis=0, keepdims=True))
        total = jnp.sum(jnp.exp(logits - top), axis=0, keepdims=True)
        stat[0] = top
        stat[1] = jnp.where(j == 0, 0.0, stat[1]) * jnp.exp(old - top) * fresh + total
        stat[2] = jnp.where(j == 0, 0.0, stat[2]) + hit

    me = z * 2 + c

    def stat_copy(slot, to, who):
        return send(
            stat_out.at[slot],
            stat_in.at[me],
            stat_send.at[slot, to],
            stat_recv.at[me],
            {"seq": origin(slot), "vocab": who},
        )

    def give(first):
        per = LANES // (2 * slots)
        for i in range(2 * STEP):
            at = pl.ds(i // per * LANES, LANES)
            back = i % per * 2 * slots
            msg = jnp.zeros((1, LANES), F32)
            for n in range(3):
                got = pltpu.roll(stat[n][:, at.start : at.start + LANES], (LANES + n * 2 * slots - back) % LANES, 1)
                inside = (lane >= n * 2 * slots) & (lane < (n + 1) * 2 * slots)
                msg = jnp.where(inside, got, msg)
            stat_out[first + i] = msg
            if i == 2 * STEP - 1:

                @pl.when(first + i == own)
                def _():
                    stat_in[me] = msg

        for i in range(2 * STEP):
            stat_copy(first + i, 1, 1 - c).start()
            if i < 2 * STEP - 1:
                stat_copy(first + i, 0, c).start()
            else:

                @pl.when(first + i != own)
                def _():
                    stat_copy(first + i, 0, c).start()

    def nrm_step(i, carry):
        s = i + 1

        @pl.when(s <= half)
        def _():
            for n in range(2):
                nrm_copy(own, up(s), n, z_up).wait_recv()

                @pl.when(s < half)
                def _():
                    nrm_copy(up(s), up(s + 1), n, z_up).start()
                    nrm_copy(own, down(s), n, z_down).wait_recv()

                @pl.when(s < half - 1)
                def _():
                    nrm_copy(down(s), down(s + 1), n, z_down).start()

            mate_copy(up(s), c).start()

            @pl.when(s < half)
            def _():
                mate_copy(down(s), c).start()

        @pl.when(s > STEP)
        def _():
            j = (s - 1) % STEP
            first = ((s - 1) // STEP - 1) * (2 * STEP)

            @pl.when(j == 0)
            def _():
                for t in range(2 * STEP):
                    mate_copy(first + t, 1 - c).wait_recv()

            scored(first, j)

            @pl.when(j == STEP - 1)
            def _():
                give(first)

        return carry

    lax.fori_loop(0, half + STEP, nrm_step, 0)

    def stat_wait(k, carry):
        @pl.when(k != me)
        def _():
            send(stat_out.at[0], stat_in.at[k], stat_send.at[0, 0], stat_recv.at[k], mate).wait_recv()

        return carry

    lax.fori_loop(0, 2 * nz, stat_wait, 0)
    two = 2 * slots
    got = stat_in[...]
    m_all = jnp.max(got, axis=0)
    mid = (lane >= two) & (lane < 2 * two)
    m_mid = pltpu.roll(m_all, two, 1)
    sums = jnp.zeros((1, LANES), F32)
    for k in range(2 * nz):
        one = got[k]
        grow = jnp.where(mid, pltpu.roll(one, two, 1) - m_mid, 0.0)
        sums = sums + one * jnp.exp(grow)
    hits = pltpu.roll(sums, LANES - 2 * two, 1)
    exps = pltpu.roll(sums, LANES - two, 1)
    inside = lane < two
    logprob = hits - (m_all + jnp.log(jnp.where(inside, exps, 1.0)))
    spot = pltpu.roll(own_info, LANES - two, 1)
    limit = jnp.where(lane < slots, len_ref[0], len_ref[1])
    ok = inside & (spot >= 0) & (spot < limit)
    tokens = jnp.where(ok, logprob, 0.0)
    tok_ref[0:1, :] = tokens[:, :slots]
    tok_ref[1:2, :] = pltpu.roll(tokens, LANES - slots, 1)[:, :slots]

    r0, r1 = rew_ref[0].astype(F32), rew_ref[1].astype(F32)
    rewards = jnp.where(lane % two < slots, r0, r1)
    mine = jnp.where(inside, tokens, jnp.where(lane < 2 * two, rewards, 0.0))
    line[...] = mine
    x_in[0] = mine

    def x_copy(d):
        where = {"sample": lax.rem(x + d, nx)}
        return send(line, x_in.at[nx - d], x_send.at[d], x_recv.at[nx - d], where)

    for d in range(1, nx):
        x_copy(d).start()
    for d in range(1, nx):
        x_copy(d).wait_recv()
    all_tok = jnp.zeros((1, LANES), F32)
    all_rew = jnp.zeros((1, LANES), F32)
    for k in range(nx):
        d = lax.rem(k + nx - x, nx)
        here = (lane >= k * two) & (lane < (k + 1) * two)
        one = x_in[d]
        all_tok = jnp.where(here, pltpu.roll(one, k * two, 1), all_tok)
        all_rew = jnp.where(here, pltpu.roll(one, (LANES + k * two - two) % LANES, 1), all_rew)
    z_out[...] = all_tok
    z_in[z] = all_tok

    def z_copy(d):
        where = {"seq": lax.rem(z + d, nz)}
        return send(z_out, z_in.at[z], z_send.at[d], z_recv.at[z], where)

    def z_start(d, carry):
        z_copy(d).start()
        return carry

    def z_wait(d, carry):
        k = lax.rem(z + d, nz)
        send(z_out, z_in.at[k], z_send.at[d], z_recv.at[k], {"seq": k}).wait()
        return carry

    lax.fori_loop(1, nz, z_start, 0)

    for n in range(2):
        for k in range(nz - 1):
            kv_copy(own, k, n, z_up).wait_send()
            nrm_copy(own, k, n, z_up).wait_send()
    for k in range(nz):
        mate_copy(k, c).wait_send()
        stat_copy(k, 1, 1 - c).wait_send()
        if k != own:
            stat_copy(k, 0, c).wait_send()
    for copy in to_right + to_left + [pass_right, pass_left, swap]:
        copy.wait_send()
    for d in range(1, nx):
        x_copy(d).wait_send()
    lax.fori_loop(1, nz, z_wait, 0)

    total = jnp.sum(z_in[...], axis=0)
    count = 2 * nx
    reward_sum = jnp.sum(all_rew, axis=1, keepdims=True) / slots
    gain = all_rew - (reward_sum - all_rew) / (count - 1)
    score = total / full_len
    obj_ref[...] = -(jnp.sum(gain * score, axis=1, keepdims=True) / count)
    parts = [
        jnp.sum(jnp.where(lane // slots == 2 * x + e, score, 0.0), axis=1, keepdims=True)
        for e in range(2)
    ]
    advs = [r - (reward_sum - r) / (count - 1) for r in (r0, r1)]
    pair = lax.broadcasted_iota(jnp.int32, (1, 2), 1)
    seq_ref[...] = jnp.where(pair == 0, parts[0], parts[1])
    adv_ref[...] = jnp.where(pair == 0, advs[0], advs[1])


def shards(
    nz,
    nx,
    queries,
    key_states,
    value_states,
    residual,
    out_weight,
    norm_gain,
    vocab_head,
    targets,
    scored_slots,
    lengths,
    rewards,
):
    count, block_len, q_width = queries.shape
    width = out_weight.shape[1]
    rows = vocab_head.shape[0]
    full_len = targets.shape[1]
    slots = scored_slots.shape[1] // nz
    heads = q_width // HD * slots
    spots = scored_slots.reshape(count, nz, slots)
    first = (jnp.arange(nz, dtype=jnp.int32) * block_len)[None, :, None]
    local = jnp.clip(spots - first, 0, block_len - 1)
    hot = local[..., None] == jnp.arange(block_len, dtype=jnp.int32)
    want = jnp.sum(jnp.where(hot, targets.reshape(count, nz, 1, block_len), 0), axis=-1)
    info = jnp.stack([want, spots]).transpose(2, 0, 1, 3).reshape(nz, 1, 2 * count * slots)
    info = jnp.pad(info, ((0, 0), (0, 0), (0, LANES - info.shape[2])))

    vmem, smem, hbm = (
        pl.BlockSpec(memory_space=pltpu.VMEM),
        pl.BlockSpec(memory_space=pltpu.SMEM),
        pl.BlockSpec(memory_space=pl.ANY),
    )
    dma = pltpu.SemaphoreType.DMA
    tokens, scores, advs, objective = pl.pallas_call(
        functools.partial(kernel, nz, nx, full_len),
        out_shape=(
            jax.ShapeDtypeStruct((count, slots), F32),
            jax.ShapeDtypeStruct((1, count), F32),
            jax.ShapeDtypeStruct((1, count), F32),
            jax.ShapeDtypeStruct((1, 1), F32),
        ),
        in_specs=[vmem, smem, smem, vmem] + [hbm] * 6,
        out_specs=(vmem,) * 4,
        scratch_shapes=[
            pltpu.VMEM(queries.shape, BF16),
            pltpu.VMEM(residual.shape[1:], BF16),
            pltpu.VMEM(out_weight.shape, BF16),
            pltpu.VMEM((nx, rows, width), BF16),
            pltpu.VMEM((nz, 2, count, block_len, HD), BF16),
            pltpu.VMEM((nz, count, slots, width), BF16),
            pltpu.VMEM((count, heads, HD), BF16),
            pltpu.VMEM((slots, width), F32),
            pltpu.VMEM((count, heads, HD), F32),
            pltpu.VMEM((count, heads, HD), F32),
            pltpu.VMEM((count, heads, HD), F32),
            pltpu.VMEM((count, slots, width), F32),
            pltpu.VMEM((slots, width), F32),
            pltpu.VMEM((3, 1, 2 * STEP * count * slots), F32),
            pltpu.VMEM((nz, 1, LANES), F32),
            pltpu.VMEM((2 * nz, 1, LANES), F32),
            pltpu.VMEM((1, LANES), F32),
            pltpu.VMEM((nx, 1, LANES), F32),
            pltpu.VMEM((1, LANES), F32),
            pltpu.VMEM((nz, 1, LANES), F32),
            dma((6,)),
            dma((6,)),
            dma((6,)),
            dma((nz, 2)),
            dma((nz, 2)),
            dma((nz, 2)),
            dma((nz, 2)),
            dma((nz,)),
            dma((nz,)),
            dma,
            dma,
            dma((nz, 2)),
            dma((2 * nz,)),
            dma((nx,)),
            dma((nx,)),
            dma((nz,)),
            dma((nz,)),
        ],
        compiler_params=pltpu.CompilerParams(collective_id=0, has_side_effects=True),
    )(
        info,
        lengths,
        rewards,
        norm_gain.reshape(1, width),
        queries,
        key_states,
        value_states,
        residual,
        out_weight,
        vocab_head,
    )
    return (tokens, scores.reshape(count), advs.reshape(count), objective.reshape(1))


def solution(mesh):
    in_specs = (
        P(("groups", "sample"), "seq", "vocab"),
        P(("groups", "sample"), "seq", "vocab"),
        P(("groups", "sample"), "seq", "vocab"),
        P(("groups", "sample"), "seq", None),
        P("vocab", None),
        P(),
        P(("seq", "sample", "vocab"), None),
        P(("groups", "sample"), None),
        P(("groups", "sample"), None),
        P(("groups", "sample")),
        P(("groups", "sample")),
    )
    out_specs = (
        P(("groups", "sample"), "seq"),
        P(("groups", "sample")),
        P(("groups", "sample")),
        P("groups"),
    )
    body = functools.partial(shards, mesh.shape["seq"], mesh.shape["sample"])
    return jax.shard_map(body, mesh=mesh, in_specs=in_specs, out_specs=out_specs, check_vma=False)
```

```python
import functools

import jax
import jax.numpy as jnp
from jax import lax
from jax.experimental import pallas as pl
from jax.experimental.pallas import tpu as pltpu
from jax.sharding import PartitionSpec as P

HD = 128
LANES = 128
STEP = 4
LEAP = 8
FLOOR = -1e30
NT = (((1,), (1,)), ((), ()))
MESH = pl.DeviceIdType.MESH
F32 = jnp.float32
BF16 = jnp.bfloat16


def kernel(
    nz,
    nx,
    full_len,
    target_ref,
    slot_ref,
    len_ref,
    rew_ref,
    gain_ref,
    q_hbm,
    k_hbm,
    v_hbm,
    res_hbm,
    w_hbm,
    head_hbm,
    tok_ref,
    seq_ref,
    adv_ref,
    obj_ref,
    info_ref,
    q_buf,
    res_buf,
    w_buf,
    head,
    kv,
    nrm,
    q_rows,
    res_rows,
    top_buf,
    sum_buf,
    acc_buf,
    part,
    part_in,
    stat,
    stat_out,
    stat_in,
    line,
    x_in,
    z_out,
    z_in,
    load_sem,
    head_send,
    head_recv,
    kv_send,
    kv_recv,
    nrm_send,
    nrm_recv,
    nrm_mate,
    part_send,
    part_recv,
    stat_send,
    stat_recv,
    x_send,
    x_recv,
    z_send,
    z_recv,
):
    z = lax.axis_index("seq")
    x = lax.axis_index("sample")
    c = lax.axis_index("vocab")
    half = nz // 2
    own = 0
    block_len = q_buf.shape[1]
    slots = nrm.shape[2]
    group = q_buf.shape[2] // HD
    width = nrm.shape[3]
    rows = head.shape[1]
    cut = width // 2
    z_up, z_down = lax.rem(z + 1, nz), lax.rem(z + nz - 1, nz)
    mate = {"vocab": 1 - c}

    near = LEAP - 1
    far_steps = half - near

    def near_slot(i):
        return 4 * (i - 1) + 1

    def far_slot(i):
        return jnp.where(i <= near, 4 * (i - 1) + 3, 4 * near + 2 * (i - 1 - near) + 1)

    def offset(slot):
        slot = slot - 1
        wide = slot < 4 * near
        i = jnp.where(wide, slot // 4 + 1, near + 1 + (slot - 4 * near) // 2)
        return jnp.where(wide & (slot % 4 < 2), i, near + i)

    def send(src, dst, send_sem, recv_sem, where):
        return pltpu.make_async_remote_copy(
            src_ref=src,
            dst_ref=dst,
            send_sem=send_sem,
            recv_sem=recv_sem,
            device_id=where,
            device_id_type=MESH,
        )

    loads = [
        pltpu.make_async_copy(k_hbm, kv.at[own, 0], load_sem.at[0]),
        pltpu.make_async_copy(v_hbm, kv.at[own, 1], load_sem.at[1]),
        pltpu.make_async_copy(head_hbm, head.at[0], load_sem.at[2]),
        pltpu.make_async_copy(q_hbm, q_buf, load_sem.at[3]),
        pltpu.make_async_copy(res_hbm.at[c], res_buf, load_sem.at[4]),
        pltpu.make_async_copy(w_hbm, w_buf, load_sem.at[5]),
    ]
    for load in loads:
        load.start()
    barrier = pltpu.get_barrier_semaphore()
    z_far, z_back = lax.rem(z + LEAP, nz), lax.rem(z + nz - LEAP, nz)
    peers = [mate]
    peers += [{"seq": there} for there in (z_up, z_down, z_far, z_back)]
    peers += [{"sample": lax.rem(x + d, nx)} for d in range(1, nx)]
    for peer in peers:
        pl.semaphore_signal(barrier, inc=1, device_id=peer, device_id_type=MESH)
    pl.semaphore_wait(barrier, len(peers))

    def kv_copy(src, dst, n, there):
        return send(
            kv.at[src, n], kv.at[dst, n], kv_send.at[dst, n], kv_recv.at[dst, n], {"seq": there}
        )

    for n in range(2):
        loads[n].wait()
        for dst, there in enumerate((z_up, z_down, z_far, z_back), 1):
            kv_copy(own, dst, n, there).start()

    hx = rows // 2
    right, left = {"sample": lax.rem(x + 1, nx)}, {"sample": lax.rem(x + nx - 1, nx)}

    def head_copy(src, dst, lo, n, where):
        return send(
            head.at[src, pl.ds(lo, hx)],
            head.at[dst, pl.ds(lo, hx)],
            head_send.at[n],
            head_recv.at[n],
            where,
        )

    loads[2].wait()
    to_right = [head_copy(0, 3, 0, 0, right), head_copy(0, 3, hx, 1, right)]
    to_left = [head_copy(0, 1, hx, 2, left), head_copy(0, 1, 0, 3, left)]
    pass_right = head_copy(3, 2, 0, 4, right)
    pass_left = head_copy(1, 2, hx, 5, left)
    for a, b in zip(to_right, to_left):
        a.start()
        b.start()

    lane = lax.broadcasted_iota(jnp.int32, (1, LANES), 1)
    near_lane = lax.broadcasted_iota(jnp.int32, (slots, LANES), 1)
    near_row = lax.broadcasted_iota(jnp.int32, (slots, LANES), 0)
    line_slots = LANES // slots
    line_blocks = LANES // block_len

    def spots_of(b, e):
        at = pl.ds(pl.multiple_of(b // line_slots * LANES, LANES), LANES)
        whole = slot_ref[e : e + 1, at]
        want = near_row + b % line_slots * slots
        return jnp.sum(jnp.where(near_lane == want, whole, 0), axis=1, keepdims=True)

    def note(b):
        at = pl.ds(pl.multiple_of(b // line_blocks * LANES, LANES), LANES)
        out = jnp.zeros((1, LANES), jnp.int32)
        for e in range(2):
            spot = spots_of(b, e)
            place = jnp.clip(spot - b * block_len, 0, block_len - 1)
            place = place + b % line_blocks * block_len
            got = jnp.where(near_lane == place, target_ref[e : e + 1, at], 0)
            got = jnp.sum(got, axis=1, keepdims=True)
            line_e = jnp.where(near_lane == near_row + e * slots, got, 0)
            line_e += jnp.where(near_lane == near_row + (2 + e) * slots, spot, 0)
            out += jnp.sum(line_e, axis=0, keepdims=True)
        info_ref[b] = out


    def picker(e):
        spot = spots_of(z, e)
        local = jnp.clip(spot - z * block_len, 0, block_len - 1)
        hot = lax.broadcasted_iota(jnp.int32, (slots, block_len), 1) == local
        return hot.astype(F32).astype(BF16), local

    picks = [picker(e) for e in range(2)]
    loads[3].wait()
    for e in range(2):
        rows_e = jnp.dot(picks[e][0], q_buf[e], preferred_element_type=F32).astype(BF16)
        for h in range(group):
            q_rows[e, pl.ds(h * slots, slots), :] = rows_e[:, h * HD : (h + 1) * HD]
    loads[4].wait()
    own_pick = jnp.where(c == 0, picks[0][0].astype(F32), picks[1][0].astype(F32)).astype(BF16)
    res_rows[...] = jnp.dot(own_pick, res_buf[...], preferred_element_type=F32)

    scale = HD ** (-0.5)
    for e in range(2):
        s0 = lax.dot_general(q_rows[e], kv[own, 0, e], NT, preferred_element_type=F32) * scale
        spot = jnp.concatenate([picks[e][1]] * group, axis=0)
        ok = lax.broadcasted_iota(jnp.int32, s0.shape, 1) <= spot
        s0 = jnp.where(ok, s0, FLOOR)
        top = jnp.max(s0, axis=1, keepdims=True)
        w0 = jnp.where(ok, jnp.exp(s0 - top), 0.0)
        top_buf[e] = jnp.broadcast_to(top, top_buf.shape[1:])
        sum_buf[e] = jnp.broadcast_to(jnp.sum(w0, axis=1, keepdims=True), sum_buf.shape[1:])
        acc_buf[e] = jnp.dot(w0.astype(BF16), kv[own, 1, e], preferred_element_type=F32)

    def attend(first):
        span = 2 * STEP * block_len
        piece = lax.broadcasted_iota(jnp.int32, (1, span), 1) // block_len
        off = offset(first + piece)
        is_up = (first + piece) % 2 == 1
        off = jnp.where(first + piece == own, nz, off)
        ok = jnp.where(is_up, off - z, jnp.where(off < half, nz - z - off, 1)) <= 0
        for e in range(2):
            keys = kv[pl.ds(first, 2 * STEP), 0, e].reshape(span, HD)
            vals = kv[pl.ds(first, 2 * STEP), 1, e].reshape(span, HD)
            sc = lax.dot_general(q_rows[e], keys, NT, preferred_element_type=F32) * scale
            sc = jnp.where(ok, sc, FLOOR)
            old = top_buf[e][:, :1]
            top = jnp.maximum(old, jnp.max(sc, axis=1, keepdims=True))
            wt = jnp.exp(sc - top)
            fade = jnp.exp(old - top)
            total = sum_buf[e][:, :1] * fade + jnp.sum(wt, axis=1, keepdims=True)
            acc_buf[e] = acc_buf[e] * fade + jnp.dot(
                wt.astype(BF16), vals, preferred_element_type=F32
            )
            top_buf[e] = jnp.broadcast_to(top, top_buf.shape[1:])
            sum_buf[e] = jnp.broadcast_to(total, sum_buf.shape[1:])

    def carry_on(i, copy, hand):
        def take(slot, nxt, last, n, there):
            copy(own, slot, n, there).wait_recv()

            @pl.when(jnp.logical_not(last))
            def _():
                copy(slot, nxt, n, there).start()

            if hand is not None:
                hand(slot, c, n).start()

        @pl.when(i <= near)
        def _():
            at, nxt = near_slot(i), near_slot(i + 1)
            for n in range(2):
                take(at, nxt, i == near, n, z_up)
                take(at + 1, nxt + 1, i == near, n, z_down)

        at, nxt = far_slot(i), far_slot(i + 1)
        for n in range(2):
            take(at, nxt, i == far_steps, n, z_up)

            @pl.when(i < far_steps)
            def _():
                take(at + 1, nxt + 1, i == far_steps - 1, n, z_down)

    per_step = (nz + far_steps - 1) // far_steps

    def kv_step(k, carry):
        i = k + 1

        carry_on(i, kv_copy, None)

        @pl.when(i == near - 2)
        def _():
            to_right[0].wait_recv()
            pass_right.start()
            to_left[0].wait_recv()
            pass_left.start()

        for t in range(per_step):

            @pl.when(k * per_step + t < nz)
            def _():
                note(k * per_step + t)

        filled = jnp.where(i <= near, 4 * i, 2 * i + 2 * near)

        @pl.when(filled % (2 * STEP) == 0)
        def _():
            attend(filled - 2 * STEP)

        return carry

    lax.fori_loop(0, far_steps, kv_step, 0)
    far_info = info_ref[lax.rem(z + half, nz)]

    sides = []
    for e in range(2):
        att = (acc_buf[e] / sum_buf[e]).astype(BF16)
        sides.append(
            jnp.concatenate([att[h * slots : (h + 1) * slots] for h in range(group)], axis=1)
        )
    loads[5].wait()
    both = jnp.dot(jnp.concatenate(sides, axis=0), w_buf[...], preferred_element_type=F32)
    for e in range(2):
        part[e] = both[e * slots : (e + 1) * slots]
    swap = send(part.at[1 - c], part_in, part_send, part_recv, mate)
    swap.start()
    hidden = res_rows[...] + part[c]
    swap.wait_recv()
    hidden = hidden + part_in[...]
    power = jnp.mean(hidden * hidden, axis=1, keepdims=True)
    nrm[own, c] = (hidden * lax.rsqrt(power + 1e-06) * gain_ref[...].reshape(1, width)).astype(BF16)

    def nrm_copy(src, dst, n, there):
        at = pl.ds(n * cut, cut)
        return send(
            nrm.at[src, c, :, at],
            nrm.at[dst, c, :, at],
            nrm_send.at[dst, n],
            nrm_recv.at[dst, c, n],
            {"seq": there},
        )

    def nrm_hand(slot, who, n):
        here = nrm.at[slot, who, :, pl.ds(n * cut, cut)]
        return send(here, here, nrm_mate.at[slot, n], nrm_recv.at[slot, who, n], mate)

    for n in range(2):
        for dst, there in enumerate((z_up, z_down, z_far, z_back), 1):
            nrm_copy(own, dst, n, there).start()
        nrm_hand(own, c, n).start()

    def origin(slot):
        off = jnp.where(slot == own, 0, offset(slot))
        move = jnp.where(slot % 2 == 1, nz - off, off)
        return lax.rem(z + move, nz)

    def scored(first, j):
        batch = nrm[pl.ds(first, 2 * STEP)].reshape(2 * STEP * 2 * slots, width)
        logits = lax.dot_general(head[j], batch, NT, preferred_element_type=F32)
        base = ((z * nx + lax.rem(x + j, nx)) * 2 + c) * rows
        ids = lax.broadcasted_iota(jnp.int32, logits.shape, 0) + base
        want = []
        per = LANES // (2 * slots)
        for t in range(2 * STEP // per):
            lines = info_ref[origin(first + t * per)]
            for i in range(1, per):
                moved = pltpu.roll(info_ref[origin(first + t * per + i)], i * 2 * slots, 1)
                lines = jnp.where(lane < i * 2 * slots, lines, moved)
            want.append(lines)
        want = jnp.concatenate(want, axis=1)
        hit = jnp.sum(jnp.where(ids == want, logits, 0.0), axis=0, keepdims=True)
        fresh = jnp.where(j == 0, 0.0, 1.0)
        old = jnp.where(j == 0, FLOOR, stat[0])
        top = jnp.maximum(old, jnp.max(logits, axis=0, keepdims=True))
        total = jnp.sum(jnp.exp(logits - top), axis=0, keepdims=True)
        stat[0] = top
        stat[1] = jnp.where(j == 0, 0.0, stat[1]) * jnp.exp(old - top) * fresh + total
        stat[2] = jnp.where(j == 0, 0.0, stat[2]) + hit

    me = z * 2 + c

    def stat_copy(slot, to, who):
        return send(
            stat_out.at[slot],
            stat_in.at[me],
            stat_send.at[slot, to],
            stat_recv.at[me],
            {"seq": lax.rem(origin(slot) + half, nz), "vocab": who},
        )

    def give(first):
        per = LANES // (2 * slots)
        for i in range(2 * STEP):
            at = pl.ds(i // per * LANES, LANES)
            back = i % per * 2 * slots
            msg = jnp.zeros((1, LANES), F32)
            for n in range(3):
                got = pltpu.roll(stat[n][:, at.start : at.start + LANES], (LANES + n * 2 * slots - back) % LANES, 1)
                inside = (lane >= n * 2 * slots) & (lane < (n + 1) * 2 * slots)
                msg = jnp.where(inside, got, msg)
            stat_out[first + i] = msg
            if i == 2 * STEP - 1:

                @pl.when(first + i == nz - 1)
                def _():
                    stat_in[me] = msg

        for i in range(2 * STEP):
            stat_copy(first + i, 1, 1 - c).start()
            if i < 2 * STEP - 1:
                stat_copy(first + i, 0, c).start()
            else:

                @pl.when(first + i != nz - 1)
                def _():
                    stat_copy(first + i, 0, c).start()

    def piece(p, carry):
        @pl.when(p == 0)
        def _():
            to_right[1].wait_recv()
            to_left[1].wait_recv()
            pass_right.wait_recv()
            pass_left.wait_recv()

        first = p // STEP * (2 * STEP)

        @pl.when(p % STEP == 0)
        def _():
            for t in range(2 * STEP):
                for n in range(2):
                    nrm_hand(first + t, 1 - c, n).wait_recv()

        scored(first, p % STEP)

        @pl.when(p % STEP == STEP - 1)
        def _():
            give(first)

        return carry

    pieces = nz // (2 * STEP) * STEP

    def due(i):
        ready = jnp.clip(2 * (i - 2), 0, pieces - STEP)
        return jnp.where(i > far_steps, pieces, ready)

    def nrm_step(k, carry):
        i = k + 1

        @pl.when(i <= far_steps)
        def _():
            carry_on(i, nrm_copy, nrm_hand)

        lax.fori_loop(due(i - 1), due(i), piece, 0)
        return carry

    lax.fori_loop(0, far_steps + 1, nrm_step, 0)

    def stat_wait(k, carry):
        @pl.when(k != me)
        def _():
            send(stat_out.at[0], stat_in.at[k], stat_send.at[0, 0], stat_recv.at[k], mate).wait_recv()

        return carry

    lax.fori_loop(0, 2 * nz, stat_wait, 0)
    two = 2 * slots
    got = stat_in[...]
    m_all = jnp.max(got, axis=0)
    mid = (lane >= two) & (lane < 2 * two)
    m_mid = pltpu.roll(m_all, two, 1)
    sums = jnp.zeros((1, LANES), F32)
    for k in range(2 * nz):
        one = got[k]
        grow = jnp.where(mid, pltpu.roll(one, two, 1) - m_mid, 0.0)
        sums = sums + one * jnp.exp(grow)
    hits = pltpu.roll(sums, LANES - 2 * two, 1)
    exps = pltpu.roll(sums, LANES - two, 1)
    inside = lane < two
    logprob = hits - (m_all + jnp.log(jnp.where(inside, exps, 1.0)))
    spot = pltpu.roll(far_info, LANES - two, 1)
    limit = jnp.where(lane < slots, len_ref[0], len_ref[1])
    ok = inside & (spot >= 0) & (spot < limit)
    tokens = jnp.where(ok, logprob, 0.0)

    r0, r1 = rew_ref[0].astype(F32), rew_ref[1].astype(F32)
    rewards = jnp.where(lane % two < slots, r0, r1)
    mine = jnp.where(inside, tokens, jnp.where(lane < 2 * two, rewards, 0.0))
    line[...] = mine
    x_in[0] = mine

    def x_copy(d):
        where = {"sample": lax.rem(x + d, nx)}
        return send(line, x_in.at[nx - d], x_send.at[d], x_recv.at[nx - d], where)

    for d in range(1, nx):
        x_copy(d).start()
    for d in range(1, nx):
        x_copy(d).wait_recv()
    all_tok = jnp.zeros((1, LANES), F32)
    all_rew = jnp.zeros((1, LANES), F32)
    for k in range(nx):
        d = lax.rem(k + nx - x, nx)
        here = (lane >= k * two) & (lane < (k + 1) * two)
        one = x_in[d]
        all_tok = jnp.where(here, pltpu.roll(one, k * two, 1), all_tok)
        all_rew = jnp.where(here, pltpu.roll(one, (LANES + k * two - two) % LANES, 1), all_rew)
    z_out[...] = all_tok
    z_in[z] = all_tok

    def z_copy(d):
        where = {"seq": lax.rem(z + d, nz)}
        return send(z_out, z_in.at[z], z_send.at[d], z_recv.at[z], where)

    def z_start(d, carry):
        z_copy(d).start()
        return carry

    def z_wait(d, carry):
        k = lax.rem(z + d, nz)
        send(z_out, z_in.at[k], z_send.at[d], z_recv.at[k], {"seq": k}).wait()
        return carry

    lax.fori_loop(1, nz, z_start, 0)

    def drain(k, carry):
        for n in range(2):
            nrm_hand(k, c, n).wait_send()

            @pl.when(k > 0)
            def _():
                kv_copy(own, k, n, z_up).wait_send()
                nrm_copy(own, k, n, z_up).wait_send()

        return carry

    lax.fori_loop(0, nz, drain, 0)
    for k in range(nz):
        stat_copy(k, 1, 1 - c).wait_send()
        if k != nz - 1:
            stat_copy(k, 0, c).wait_send()
    for copy in to_right + to_left + [pass_right, pass_left, swap]:
        copy.wait_send()
    for d in range(1, nx):
        x_copy(d).wait_send()
    lax.fori_loop(1, nz, z_wait, 0)

    back = pltpu.roll(z_in[lax.rem(z + half, nz)], LANES - x * two, 1)
    tok_ref[0:1, :] = back[:, :slots]
    tok_ref[1:2, :] = pltpu.roll(back, LANES - slots, 1)[:, :slots]
    total = jnp.sum(z_in[...], axis=0)
    count = 2 * nx
    reward_sum = jnp.sum(all_rew, axis=1, keepdims=True) / slots
    gain = all_rew - (reward_sum - all_rew) / (count - 1)
    score = total / full_len
    obj_ref[...] = -(jnp.sum(gain * score, axis=1, keepdims=True) / count)
    parts = [
        jnp.sum(jnp.where(lane // slots == 2 * x + e, score, 0.0), axis=1, keepdims=True)
        for e in range(2)
    ]
    advs = [r - (reward_sum - r) / (count - 1) for r in (r0, r1)]
    pair = lax.broadcasted_iota(jnp.int32, (1, 2), 1)
    seq_ref[...] = jnp.where(pair == 0, parts[0], parts[1])
    adv_ref[...] = jnp.where(pair == 0, advs[0], advs[1])


def shards(
    nz,
    nx,
    queries,
    key_states,
    value_states,
    residual,
    out_weight,
    norm_gain,
    vocab_head,
    targets,
    scored_slots,
    lengths,
    rewards,
):
    count, block_len, q_width = queries.shape
    width = out_weight.shape[1]
    rows = vocab_head.shape[0]
    full_len = targets.shape[1]
    slots = scored_slots.shape[1] // nz
    heads = q_width // HD * slots
    vmem, smem, hbm = (
        pl.BlockSpec(memory_space=pltpu.VMEM),
        pl.BlockSpec(memory_space=pltpu.SMEM),
        pl.BlockSpec(memory_space=pl.ANY),
    )
    dma = pltpu.SemaphoreType.DMA
    tokens, scores, advs, objective = pl.pallas_call(
        functools.partial(kernel, nz, nx, full_len),
        out_shape=(
            jax.ShapeDtypeStruct((count, slots), F32),
            jax.ShapeDtypeStruct((1, count), F32),
            jax.ShapeDtypeStruct((1, count), F32),
            jax.ShapeDtypeStruct((1, 1), F32),
        ),
        in_specs=[vmem, vmem, smem, smem, vmem] + [hbm] * 6,
        out_specs=(vmem,) * 4,
        scratch_shapes=[
            pltpu.VMEM((nz, 1, LANES), jnp.int32),
            pltpu.VMEM(queries.shape, BF16),
            pltpu.VMEM(residual.shape[1:], BF16),
            pltpu.VMEM(out_weight.shape, BF16),
            pltpu.VMEM((nx, rows, width), BF16),
            pltpu.VMEM((nz, 2, count, block_len, HD), BF16),
            pltpu.VMEM((nz, count, slots, width), BF16),
            pltpu.VMEM((count, heads, HD), BF16),
            pltpu.VMEM((slots, width), F32),
            pltpu.VMEM((count, heads, HD), F32),
            pltpu.VMEM((count, heads, HD), F32),
            pltpu.VMEM((count, heads, HD), F32),
            pltpu.VMEM((count, slots, width), F32),
            pltpu.VMEM((slots, width), F32),
            pltpu.VMEM((3, 1, 2 * STEP * count * slots), F32),
            pltpu.VMEM((nz, 1, LANES), F32),
            pltpu.VMEM((2 * nz, 1, LANES), F32),
            pltpu.VMEM((1, LANES), F32),
            pltpu.VMEM((nx, 1, LANES), F32),
            pltpu.VMEM((1, LANES), F32),
            pltpu.VMEM((nz, 1, LANES), F32),
            dma((6,)),
            dma((6,)),
            dma((6,)),
            dma((nz, 2)),
            dma((nz, 2)),
            dma((nz, 2)),
            dma((nz, 2, 2)),
            dma((nz, 2)),
            dma,
            dma,
            dma((nz, 2)),
            dma((2 * nz,)),
            dma((nx,)),
            dma((nx,)),
            dma((nz,)),
            dma((nz,)),
        ],
        compiler_params=pltpu.CompilerParams(collective_id=0, has_side_effects=True),
    )(
        targets,
        scored_slots,
        lengths,
        rewards,
        norm_gain,
        queries,
        key_states,
        value_states,
        residual,
        out_weight,
        vocab_head,
    )
    return (tokens, scores.reshape(count), advs.reshape(count), objective.reshape(1))


def solution(mesh):
    in_specs = (
        P(("groups", "sample"), "seq", "vocab"),
        P(("groups", "sample"), "seq", "vocab"),
        P(("groups", "sample"), "seq", "vocab"),
        P(("groups", "sample"), "seq", None),
        P("vocab", None),
        P(),
        P(("seq", "sample", "vocab"), None),
        P(("groups", "sample"), None),
        P(("groups", "sample"), None),
        P(("groups", "sample")),
        P(("groups", "sample")),
    )
    out_specs = (
        P(("groups", "sample"), "seq"),
        P(("groups", "sample")),
        P(("groups", "sample")),
        P("groups"),
    )
    body = functools.partial(shards, mesh.shape["seq"], mesh.shape["sample"])
    return jax.shard_map(body, mesh=mesh, in_specs=in_specs, out_specs=out_specs, check_vma=False)
```
